32 devices in a mesh: grp: 4 (over x, core), pages: 8 (over z, y).
Axes of the slice: x: 2, y: 2, z: 4, core: 2. Of those that a mesh axis runs over, the one named last changes fastest.
Arguments:
- queries: bfloat16 [128, 64, 2048], P(('grp', 'pages')), parts along dimension 0, may hold values from -500 to 500
- tree_keys: bfloat16 [128, 64, 512], P(('grp', 'pages')), parts along dimension 0, may hold values from -6 to 6
- tree_values: bfloat16 [128, 64, 512], P(('grp', 'pages')), parts along dimension 0, may hold values from -6 to 6
- page_keys: bfloat16 [256, 256, 512], P(('grp', 'pages')), parts along dimension 0, may hold values from -6 to 6
- page_values: bfloat16 [256, 256, 512], P(('grp', 'pages')), parts along dimension 0, may hold values from -6 to 6
- page_table: int32 [128, 4], P(('grp', 'pages')), parts along dimension 0, may hold values from 0 to 63, as said below
- prefix_lengths: int32 [128], P(('grp', 'pages')), parts along dimension 0, may hold values from 513 to 1024
- tree_parents: int32 [128, 64], P(('grp', 'pages')), parts along dimension 0, may hold values from -1 to 62, as said below
- live_lengths: int32 [128], P(('grp', 'pages')), parts along dimension 0, may hold values from 1 to 64
Outputs:
- attended: bfloat16 [128, 64, 2048], P(('grp', 'pages')), parts along dimension 0
- page_reads: int32 [256], P(('grp', 'pages')), parts along dimension 0
The draws below stay inside these ranges and needn't reach their ends.
There are 4 independent parts, one for each index of `grp`. The reference program is written for one: setup_inputs(seed, part) draws one part's arguments, and reference() takes and returns one part's arrays. A program takes and returns all parts, laid end to end along the dimension named above; each array names one. Nothing has to cross between parts.
Inputs may be any that keep to these rules, and one draw needn't show every extreme that they name: `page_table`: the owner of page p is index p // 8 along pages. Over the rows of one device, the used slots name pages of any one owner at most 2 times, and in every draw each device names some owner exactly 2 times. `tree_parents`: entry t is -1 for t = 0 and a number below t otherwise.
All inputs are finite; a program needn't handle non-finite values.
Results may differ from the reference program's by a relative error of at most 0.0085.
Values may be sent and summed in bfloat16 or wider, within the bound.
A program may use at most 192 MiB of HBM per device.

```python
import jax
import jax.numpy as jnp
from jax import lax

QH = 16
KVH = 4
HD = 128
TREE = 64
PAGE = 256
MAXP = 4
REQ_DEV = 4
PAGES_DEV = 8
REQ = 32
NPAGES = 64
CAP = 2


def draw_queries(key, part):
    first = jax.random.fold_in(key, 0)
    fourth = jax.random.fold_in(key, 3)
    base = jnp.clip(jax.random.normal(first, (REQ, TREE, QH * HD), jnp.float32), -6.0, 6.0)
    moderate_amount = jnp.exp(jax.random.uniform(fourth, (REQ, TREE, 1), jnp.float32, jnp.log(0.5), jnp.log(2.0)))
    factor = moderate_amount
    return (base * factor).astype(jnp.bfloat16)


def draw_tree_parents(key, part):
    index = jnp.arange(TREE, dtype=jnp.int32)
    upper = jnp.maximum(index, 1)
    parents = jax.random.randint(key, (REQ, TREE), 0, upper[None, :], jnp.int32)
    return jnp.where(index[None, :] == 0, -1, parents).astype(jnp.int32)


def draw_page_table(key, part):
    every_owner_list = REQ // REQ_DEV
    choose = REQ_DEV * MAXP // CAP
    key_hot, key_score, key_page = jax.random.split(jax.random.fold_in(key, 7), 3)
    sorted_ranking = jax.random.permutation(key_hot, every_owner_list)
    popular_page_count = max(1, every_owner_list // 8)
    extra_reward = jnp.where(sorted_ranking < popular_page_count, 1 << 24, 0).astype(jnp.int32)
    random_jitter = jax.random.randint(key_score, (every_owner_list, every_owner_list), 0, 4096, jnp.int32)
    score_values = random_jitter * every_owner_list + jnp.arange(every_owner_list, dtype=jnp.int32)[None, :] + extra_reward[None, :]
    chosen = lax.top_k(score_values, choose)[1].astype(jnp.int32)
    local_req = jnp.arange(REQ_DEV, dtype=jnp.int32)
    slot = jnp.arange(MAXP, dtype=jnp.int32)
    group = (slot[None, :] * REQ_DEV + local_req[:, None]) // CAP
    owner = chosen[:, group].reshape(REQ, MAXP)
    local = jax.random.randint(key_page, (REQ, MAXP), 0, PAGES_DEV, jnp.int32)
    return (owner * PAGES_DEV + local).astype(jnp.int32)


def with_ends(drawn, own_key, low, high):
    index_at = [jax.random.randint(jax.random.fold_in(own_key, axis), (), 0, length) for axis, length in enumerate(drawn.shape)]
    main_axis = drawn.shape.index(max(drawn.shape))
    neighbour = index_at[:main_axis] + [(index_at[main_axis] + 1) % drawn.shape[main_axis]] + index_at[main_axis + 1:]
    return drawn.at[tuple(index_at)].set(low).at[tuple(neighbour)].set(high)


def shard_levels(own_key, extent, cuts, smallest, largest):
    factor_of = 1.0
    for position, blocks in cuts:
        draws = jax.random.uniform(jax.random.fold_in(jax.random.fold_in(own_key, 6), position), (blocks,), jnp.float32, smallest / len(cuts), largest / len(cuts))
        factor_of = factor_of * jnp.repeat(jnp.exp(draws), extent[position] // blocks).reshape((-1,) + (1,) * (len(extent) - 1 - position))
    return factor_of


def gaussian(rng, extent, scale, most, pieces=(), held_as=jnp.bfloat16):
    drawn = jax.random.normal(rng, extent, jnp.float32) * scale
    if len(pieces) > 0:
        drawn = shard_levels(rng, extent, pieces, -0.22, 0.18) * drawn
    return jnp.clip(drawn, min=-most, max=most).astype(held_as)


def setup_inputs(seed: int = 0, part: int = 0) -> dict:
    key_list = jax.random.split(jax.random.key(seed), 10)
    own_keys = jax.random.split(jax.random.fold_in(key_list[9], part), 10)
    return {
        "queries": draw_queries(jax.random.fold_in(jax.random.fold_in(key_list[9], part), 71), part),
        "tree_keys": gaussian(own_keys[1], (REQ, TREE, KVH * HD), 1.0, 6.0, ((0, 8),)),
        "tree_values": gaussian(own_keys[2], (REQ, TREE, KVH * HD), 1.0, 6.0, ((0, 8),)),
        "page_keys": gaussian(own_keys[3], (NPAGES, PAGE, KVH * HD), 1.0, 6.0, ((0, 8),)),
        "page_values": gaussian(own_keys[4], (NPAGES, PAGE, KVH * HD), 1.0, 6.0, ((0, 8),)),
        "page_table": draw_page_table(jax.random.fold_in(jax.random.fold_in(key_list[9], part), 71), part),
        "prefix_lengths": with_ends(jax.random.randint(own_keys[6], (REQ,), (MAXP // 2) * PAGE + 1, MAXP * PAGE + 1), jax.random.fold_in(own_keys[6], 1), (MAXP // 2) * PAGE + 1, MAXP * PAGE).astype(jnp.int32),
        "tree_parents": draw_tree_parents(jax.random.fold_in(jax.random.fold_in(key_list[9], part), 71), part),
        "live_lengths": with_ends(jax.random.randint(own_keys[8], (REQ,), 1, TREE + 1), jax.random.fold_in(own_keys[8], 1), 1, TREE).astype(jnp.int32),
    }


NEG_BIG = -1e30


def ancestry(parents):
    index = jnp.arange(TREE, dtype=jnp.int32)
    links = (index[None, None, :] == parents[:, :, None]) | (index[None, :, None] == index[None, None, :])
    reach = links.astype(jnp.float32)
    for level in range((TREE - 1).bit_length()):
        reach = (jnp.einsum("rts,rsu->rtu", reach, reach, precision=lax.Precision.HIGHEST) > 0).astype(jnp.float32)
    return reach


def tree_parts(queries, keys, values, reach, live):
    groups = QH // KVH
    count = queries.shape[0]
    query = queries.astype(jnp.float32).reshape(count, TREE, KVH, groups, HD)
    keyed = keys.astype(jnp.float32).reshape(count, TREE, KVH, HD)
    valued = values.astype(jnp.float32).reshape(count, TREE, KVH, HD)
    score_values = jnp.einsum("rtkgd,rskd->rkgts", query, keyed, precision=lax.Precision.HIGHEST) * HD ** -0.5
    allowed = (reach > 0) & (jnp.arange(TREE, dtype=jnp.int32)[None, None, :] < live[:, None, None])
    score_values = jnp.where(allowed[:, None, None, :, :], score_values, NEG_BIG)
    peak = jnp.max(score_values, axis=-1)
    expo = jnp.exp(score_values - peak[..., None])
    total = jnp.sum(expo, axis=-1)
    weights = lax.optimization_barrier(expo.astype(jnp.bfloat16)).astype(jnp.float32)
    out = jnp.einsum("rkgts,rskd->rtkgd", weights, valued, precision=lax.Precision.HIGHEST)
    out = out.reshape(count, TREE, QH, HD)
    peak = peak.transpose(0, 3, 1, 2).reshape(count, TREE, QH)
    total = total.transpose(0, 3, 1, 2).reshape(count, TREE, QH)
    return peak, total, out


def page_parts(query_rows, keys, values, counts):
    groups = QH // KVH
    query = query_rows.astype(jnp.float32).reshape(TREE, KVH, groups, HD)
    keyed = keys.astype(jnp.float32).reshape(MAXP, PAGE, KVH, HD)
    valued = values.astype(jnp.float32).reshape(MAXP, PAGE, KVH, HD)
    score_values = jnp.einsum("tkgd,jpkd->jkgtp", query, keyed, precision=lax.Precision.HIGHEST) * HD ** -0.5
    allowed = jnp.arange(PAGE, dtype=jnp.int32)[None, :] < counts[:, None]
    score_values = jnp.where(allowed[:, None, None, None, :], score_values, NEG_BIG)
    peak = jnp.max(score_values, axis=-1)
    expo = jnp.exp(score_values - peak[..., None])
    total = jnp.sum(expo, axis=-1)
    weights = lax.optimization_barrier(expo.astype(jnp.bfloat16)).astype(jnp.float32)
    out = jnp.einsum("jkgtp,jpkd->jtkgd", weights, valued, precision=lax.Precision.HIGHEST)
    out = out.astype(jnp.bfloat16).reshape(MAXP, TREE, QH, HD)
    peak = peak.transpose(0, 3, 1, 2).reshape(MAXP, TREE, QH)
    total = total.transpose(0, 3, 1, 2).reshape(MAXP, TREE, QH)
    return peak, total, out


def reference(queries, tree_keys, tree_values, page_keys, page_values, page_table, prefix_lengths, tree_parents, live_lengths):
    slots = jnp.arange(MAXP, dtype=jnp.int32)
    key_counts = jnp.clip(prefix_lengths[:, None] - slots[None, :] * PAGE, 0, PAGE).astype(jnp.int32)
    used = key_counts > 0
    reach = ancestry(tree_parents)
    tree_peak, tree_total, tree_out = tree_parts(queries, tree_keys, tree_values, reach, live_lengths)

    def one_request(items):
        query_rows, table_row, count_row = items
        return page_parts(query_rows, page_keys[table_row], page_values[table_row], count_row)

    page_maximum, page_total, page_out = lax.map(one_request, (queries, page_table, key_counts))
    usable = used[:, :, None, None]
    masked = jnp.where(usable, page_maximum, NEG_BIG)
    top = jnp.maximum(tree_peak, jnp.max(masked, axis=1))
    tree_scale = jnp.exp(tree_peak - top)
    page_scale = jnp.where(usable, jnp.exp(masked - top[:, None]), 0.0)
    total = tree_total * tree_scale + jnp.sum(page_scale * page_total, axis=1)
    mixed = tree_out * tree_scale[..., None] + jnp.sum(page_scale[..., None] * page_out.astype(jnp.float32), axis=1)
    attended = (mixed / total[..., None]).reshape(REQ, TREE, QH * HD).astype(jnp.bfloat16)
    weight = jnp.where(used, live_lengths[:, None], 0).astype(jnp.float32)
    reads = jax.ops.segment_sum(weight.reshape(-1), page_table.reshape(-1), num_segments=NPAGES)
    return attended, reads.astype(jnp.int32)
```

```python
import functools

import jax
import jax.numpy as jnp
from jax import lax
from jax.experimental import pallas as pl
from jax.experimental.pallas import tpu as pltpu
from jax.sharding import PartitionSpec as P

QH = 16
KVH = 4
HD = 128
GROUPS = QH // KVH
NEG_BIG = -1e30
SCALE = HD ** (-0.5)
NT = (((1,), (1,)), ((), ()))
MESH = pl.DeviceIdType.MESH


def head(h):
    return slice(h * HD, (h + 1) * HD)


def attend(query_of, keys_of, values_of, allowed, out_to, stats, lane, first):
    for k in range(KVH):
        query = jnp.concatenate([query_of(k * GROUPS + g) for g in range(GROUPS)], axis=0)
        scores = (
            lax.dot_general(query, keys_of(k), NT, preferred_element_type=jnp.float32) * SCALE
        )
        scores = jnp.where(allowed, scores, NEG_BIG)
        peak = jnp.max(scores, axis=-1, keepdims=True)
        expo = jnp.exp(scores - peak)
        total = jnp.sum(expo, axis=-1, keepdims=True)
        out = jnp.dot(
            expo.astype(jnp.bfloat16), values_of(k), preferred_element_type=jnp.float32
        )
        rows = out.shape[0] // GROUPS
        for g in range(GROUPS):
            h = k * GROUPS + g
            part = slice(g * rows, (g + 1) * rows)
            out_to(h, out[part])
            stats = jnp.where(lane == first + h, peak[part], stats)
            stats = jnp.where(lane == first + QH + h, total[part], stats)
    return stats


def exchange(
    n,
    cap,
    meta,
    live,
    q_ref,
    tk_ref,
    tv_ref,
    link_ref,
    pk_ref,
    pv_ref,
    got_out,
    got_stats,
    tree_out,
    tree_stats,
    q_all,
    q_now,
    out_send,
    stats_send,
    q_send_sem,
    q_recv_sem,
    out_send_sem,
    out_recv_sem,
    stats_send_sem,
    stats_recv_sem,
    local_sem,
):
    reqs, tree, _ = q_ref.shape
    page = pk_ref.shape[1]
    depth = n // 2
    me = lax.axis_index("pages")
    z, y = me // 2, me % 2
    other = 1 - y
    partner = z * 2 + other

    barrier = pltpu.get_barrier_semaphore()

    def greet(i, _):
        pl.semaphore_signal(
            barrier, inc=1, device_id={"pages": (me + i) % n}, device_id_type=MESH
        )
        return 0

    lax.fori_loop(1, n, greet, 0)
    pl.semaphore_wait(barrier, n - 1)

    def q_copy(src_ref, src, i, way, to):
        return pltpu.make_async_remote_copy(
            src_ref=src_ref,
            dst_ref=q_all.at[src, i],
            send_sem=q_send_sem.at[way, src // 2, i],
            recv_sem=q_recv_sem.at[src, i],
            device_id={"pages": to},
            device_id_type=MESH,
        )

    def out_copy(d):
        return pltpu.make_async_remote_copy(
            src_ref=out_send.at[d],
            dst_ref=got_out.at[me],
            send_sem=out_send_sem.at[d],
            recv_sem=out_recv_sem.at[me],
            device_id={"pages": d},
            device_id_type=MESH,
        )

    def stats_copy(d):
        return pltpu.make_async_remote_copy(
            src_ref=stats_send.at[d],
            dst_ref=got_stats.at[me],
            send_sem=stats_send_sem.at[d],
            recv_sem=stats_recv_sem.at[me],
            device_id={"pages": d},
            device_id_type=MESH,
        )

    def q_arrive(src, i):
        pltpu.make_async_remote_copy(
            src_ref=q_all.at[src, i],
            dst_ref=q_all.at[src, i],
            send_sem=q_send_sem.at[0, src // 2, i],
            recv_sem=q_recv_sem.at[src, i],
            device_id={"pages": partner},
            device_id_type=MESH,
        ).wait_recv()

    for i in range(reqs):
        q_copy(q_ref.at[i], me, i, 2, partner).start()

        @pl.when(z + 1 < depth)
        def _():
            q_copy(q_ref.at[i], me, i, 0, me + 2).start()

        @pl.when(z > 0)
        def _():
            q_copy(q_ref.at[i], me, i, 1, me - 2).start()

    lane = lax.broadcasted_iota(jnp.int32, (tree, HD), 1)
    key_lane = lax.broadcasted_iota(jnp.int32, (GROUPS * tree, page), 1)

    def serve(d):
        stats = jnp.zeros((tree, HD), jnp.float32)
        for c in range(cap):
            base = (d * cap + c) * 3
            which, count, req = meta[base], meta[base + 1], meta[base + 2]

            def out_to(h, value):
                out_send[d, c, :, head(h)] = value.astype(jnp.bfloat16)

            stats = attend(
                lambda h: q_now[req, :, head(h)],
                lambda k: pk_ref[which, :, head(k)],
                lambda k: pv_ref[which, :, head(k)],
                key_lane < count,
                out_to,
                stats,
                lane,
                c * 2 * QH,
            )
        stats_send[d] = stats

    q_now[...] = q_ref[...]
    serve(me)
    own_out = pltpu.make_async_copy(out_send.at[me], got_out.at[me], local_sem.at[0])
    own_stats = pltpu.make_async_copy(stats_send.at[me], got_stats.at[me], local_sem.at[1])
    own_out.start()
    own_stats.start()

    def one_tree(r, _):
        reach = link_ref[r]
        for level in range((tree - 1).bit_length()):
            reach = jnp.where(
                jnp.dot(reach, reach, preferred_element_type=jnp.float32) > 0, 1.0, 0.0
            ).astype(jnp.bfloat16)
        seen = lax.broadcasted_iota(jnp.int32, (tree, tree), 1) < live[r]
        open_ = jnp.where(seen, reach.astype(jnp.float32), 0.0)
        allowed = jnp.concatenate([open_] * GROUPS, axis=0) > 0

        def out_to(h, value):
            tree_out[r, :, head(h)] = value

        tree_stats[r] = attend(
            lambda h: q_ref[r, :, head(h)],
            lambda k: tk_ref[r, :, head(k)],
            lambda k: tv_ref[r, :, head(k)],
            allowed,
            out_to,
            jnp.zeros((tree, HD), jnp.float32),
            lane,
            0,
        )
        return 0

    lax.fori_loop(0, reqs, one_tree, 0)

    def step(s, _):
        for i in range(reqs):

            @pl.when(z - s >= 0)
            def _():
                src = me - 2 * s
                q_arrive(src, i)
                q_copy(q_all.at[src, i], src, i, 2, partner).start()

                @pl.when(z + 1 < depth)
                def _():
                    q_copy(q_all.at[src, i], src, i, 0, me + 2).start()

            @pl.when(z + s < depth)
            def _():
                src = me + 2 * s
                q_arrive(src, i)
                q_copy(q_all.at[src, i], src, i, 2, partner).start()

                @pl.when(z > 0)
                def _():
                    q_copy(q_all.at[src, i], src, i, 1, me - 2).start()

        def case(k, _):
            crossed = k // 2
            far = s - crossed
            row = z + far * (2 * (k % 2) - 1)
            column = y + crossed * (other - y)
            d = row * 2 + column
            valid = (row >= 0) & (row < depth) & ((far > 0) | (k == 2))

            @pl.when(valid)
            def _():
                @pl.when(crossed == 1)
                def _():
                    for i in range(reqs):
                        q_arrive(d, i)

                q_now[...] = q_all[d]
                serve(d)
                out_copy(d).start()
                stats_copy(d).start()

            return 0

        lax.fori_loop(0, 4, case, 0)
        return 0

    lax.fori_loop(1, depth + 1, step, 0)

    own_out.wait()
    own_stats.wait()

    def finish(i, _):
        d = (me + i) % n
        out_copy(d).wait_send()
        stats_copy(d).wait_send()
        pltpu.make_async_remote_copy(
            src_ref=out_send.at[d],
            dst_ref=got_out.at[d],
            send_sem=out_send_sem.at[d],
            recv_sem=out_recv_sem.at[d],
            device_id={"pages": d},
            device_id_type=MESH,
        ).wait_recv()
        pltpu.make_async_remote_copy(
            src_ref=stats_send.at[d],
            dst_ref=got_stats.at[d],
            send_sem=stats_send_sem.at[d],
            recv_sem=stats_recv_sem.at[d],
            device_id={"pages": d},
            device_id_type=MESH,
        ).wait_recv()
        return 0

    lax.fori_loop(1, n, finish, 0)

    def drain(row, _):
        src = row * 2 + y
        for i in range(reqs):
            q_copy(q_all.at[src, i], src, i, 2, partner).wait_send()

            @pl.when((row <= z) & (z + 1 < depth))
            def _():
                q_copy(q_all.at[src, i], src, i, 0, me + 2).wait_send()

            @pl.when((row >= z) & (z > 0))
            def _():
                q_copy(q_all.at[src, i], src, i, 1, me - 2).wait_send()

        return 0

    lax.fori_loop(0, depth, drain, 0)


def combine(cap, slots, target, used, tree_out, tree_stats, *refs):
    outs, stats, attended = refs[:slots], refs[slots : 2 * slots], refs[2 * slots]
    r = pl.program_id(0)
    tree_peak, tree_total = tree_stats[0, :, :QH], tree_stats[0, :, QH : 2 * QH]
    peaks, totals = [], []
    for j in range(slots):
        c = target[r * slots + j] % cap
        held = stats[j][0, :, : 2 * QH]
        for other in range(1, cap):
            held = jnp.where(
                c == other, stats[j][0, :, other * 2 * QH : (other + 1) * 2 * QH], held
            )
        peaks.append(jnp.where(used[r * slots + j] > 0, held[:, :QH], NEG_BIG))
        totals.append(held[:, QH:])
    top = tree_peak
    for peak in peaks:
        top = jnp.maximum(top, peak)
    tree_scale = jnp.exp(tree_peak - top)
    scales = [
        jnp.where(used[r * slots + j] > 0, jnp.exp(peaks[j] - top), 0.0) for j in range(slots)
    ]
    total = tree_total * tree_scale
    for j in range(slots):
        total = total + scales[j] * totals[j]
    for h in range(QH):
        mixed = tree_out[0, :, head(h)] * tree_scale[:, h : h + 1]
        for j in range(slots):
            mixed = mixed + outs[j][0, :, head(h)].astype(jnp.float32) * scales[j][:, h : h + 1]
        attended[0, :, head(h)] = (mixed / total[:, h : h + 1]).astype(jnp.bfloat16)


def shards(
    queries,
    tree_keys,
    tree_values,
    page_keys,
    page_values,
    page_table,
    prefix_lengths,
    tree_parents,
    live_lengths,
):
    n = lax.axis_size("pages")
    me = lax.axis_index("pages")
    reqs, tree, width = queries.shape
    pages_here, page_size, _ = page_keys.shape
    slots = page_table.shape[1]
    pairs = reqs * slots
    cap = max(1, pairs // n)

    mine = jnp.concatenate([page_table.reshape(-1), prefix_lengths, live_lengths])
    every = lax.all_gather(mine, "pages", axis=0, tiled=False)
    table = every[:, :pairs]
    prefix = jnp.repeat(every[:, pairs : pairs + reqs], slots, axis=1)
    lives = jnp.repeat(every[:, pairs + reqs :], slots, axis=1)
    pair = jnp.arange(pairs, dtype=jnp.int32)
    slot, req = pair % slots, pair // slots
    counts = jnp.clip(prefix - slot[None, :] * page_size, 0, page_size)
    local = table - me * pages_here
    here = (counts > 0) & (local >= 0) & (local < pages_here)
    before = pair[None, :] < pair[:, None]
    rank = jnp.sum((here[:, None, :] & before[None]).astype(jnp.int32), axis=2)
    take = here[:, None, :] & (rank[:, None, :] == jnp.arange(cap, dtype=jnp.int32)[None, :, None])
    facts = jnp.stack([local, counts, jnp.broadcast_to(req[None], local.shape)], axis=1)
    meta = jnp.sum(jnp.where(take[:, :, None, :], facts[:, None], 0), axis=3).reshape(-1)
    local_pages = jnp.arange(pages_here, dtype=jnp.int32)
    hit = here[None] & (local[None] == local_pages[:, None, None])
    reads = jnp.sum(jnp.where(hit, lives[None], 0), axis=(1, 2)).astype(jnp.int32)

    my_pages = page_table.reshape(-1)
    my_used = jnp.repeat(prefix_lengths, slots) > slot * page_size
    owners = my_pages // pages_here
    my_rank = jnp.sum(
        ((owners[:, None] == owners[None, :]) & my_used[None, :] & before).astype(jnp.int32),
        axis=1,
    )
    target = jnp.where(my_used, owners * cap + my_rank, me * cap)
    used = my_used.astype(jnp.int32)

    index = jnp.arange(tree, dtype=jnp.int32)
    links = (
        (index[None, None, :] == tree_parents[:, :, None])
        | (index[None, :, None] == index[None, None, :])
    ).astype(jnp.bfloat16)

    smem = pl.BlockSpec(memory_space=pltpu.SMEM)
    vmem = pl.BlockSpec(memory_space=pltpu.VMEM)
    hbm = pl.BlockSpec(memory_space=pl.ANY)
    depth = n // 2
    got_out, got_stats, tree_out, tree_stats = pl.pallas_call(
        functools.partial(exchange, n, cap),
        out_shape=(
            jax.ShapeDtypeStruct((n, cap, tree, width), jnp.bfloat16),
            jax.ShapeDtypeStruct((n, tree, HD), jnp.float32),
            jax.ShapeDtypeStruct((reqs, tree, width), jnp.float32),
            jax.ShapeDtypeStruct((reqs, tree, HD), jnp.float32),
        ),
        in_specs=[smem, smem] + [vmem] * 6,
        out_specs=(hbm, hbm, vmem, vmem),
        scratch_shapes=[
            pltpu.VMEM((n, reqs, tree, width), jnp.bfloat16),
            pltpu.VMEM((reqs, tree, width), jnp.bfloat16),
            pltpu.VMEM((n, cap, tree, width), jnp.bfloat16),
            pltpu.VMEM((n, tree, HD), jnp.float32),
            pltpu.SemaphoreType.DMA((3, depth, reqs)),
            pltpu.SemaphoreType.DMA((n, reqs)),
            pltpu.SemaphoreType.DMA((n,)),
            pltpu.SemaphoreType.DMA((n,)),
            pltpu.SemaphoreType.DMA((n,)),
            pltpu.SemaphoreType.DMA((n,)),
            pltpu.SemaphoreType.DMA((2,)),
        ],
        compiler_params=pltpu.CompilerParams(
            collective_id=0, has_side_effects=True, vmem_limit_bytes=62 * 1024 * 1024
        ),
        name="exchange",
    )(meta, live_lengths, queries, tree_keys, tree_values, links, page_keys, page_values)

    def own(r, *_):
        return (r, 0, 0)

    def out_at(j):
        return lambda r, target, used: (target[r * slots + j], 0, 0)

    def stats_at(j):
        return lambda r, target, used: (target[r * slots + j] // cap, 0, 0)

    got_out = got_out.reshape(n * cap, tree, width)
    attended = pl.pallas_call(
        functools.partial(combine, cap, slots),
        out_shape=jax.ShapeDtypeStruct((reqs, tree, width), jnp.bfloat16),
        grid_spec=pltpu.PrefetchScalarGridSpec(
            num_scalar_prefetch=2,
            grid=(reqs,),
            in_specs=[pl.BlockSpec((1, tree, width), own), pl.BlockSpec((1, tree, HD), own)]
            + [pl.BlockSpec((1, tree, width), out_at(j)) for j in range(slots)]
            + [pl.BlockSpec((1, tree, HD), stats_at(j)) for j in range(slots)],
            out_specs=pl.BlockSpec((1, tree, width), own),
        ),
        name="combine",
    )(target, used, tree_out, tree_stats, *([got_out] * slots), *([got_stats] * slots))
    return (attended, reads)


def solution(mesh):
    rows = P(("grp", "pages"), None, None)
    return jax.shard_map(
        shards,
        mesh=mesh,
        in_specs=(
            rows,
            rows,
            rows,
            rows,
            rows,
            P(("grp", "pages"), None),
            P(("grp", "pages")),
            P(("grp", "pages"), None),
            P(("grp", "pages")),
        ),
        out_specs=(rows, P(("grp", "pages"))),
        check_vma=False,
    )
```

```python
import functools

import jax
import jax.numpy as jnp
from jax import lax
from jax.experimental import pallas as pl
from jax.experimental.pallas import tpu as pltpu
from jax.sharding import PartitionSpec as P

QH = 16
KVH = 4
HD = 128
GROUPS = QH // KVH
NEG_BIG = -1e30
SCALE = HD ** (-0.5)
NT = (((1,), (1,)), ((), ()))
MESH = pl.DeviceIdType.MESH


def head(h):
    return slice(h * HD, (h + 1) * HD)


def attend(query_of, keys_of, values_of, allowed, out_to, stats, lane, first):
    for k in range(KVH):
        query = jnp.concatenate([query_of(k * GROUPS + g) for g in range(GROUPS)], axis=0)
        scores = (
            lax.dot_general(query, keys_of(k), NT, preferred_element_type=jnp.float32) * SCALE
        )
        scores = jnp.where(allowed, scores, NEG_BIG)
        peak = jnp.max(scores, axis=-1, keepdims=True)
        expo = jnp.exp(scores - peak)
        total = jnp.sum(expo, axis=-1, keepdims=True)
        out = jnp.dot(
            expo.astype(jnp.bfloat16), values_of(k), preferred_element_type=jnp.float32
        )
        rows = out.shape[0] // GROUPS
        for g in range(GROUPS):
            h = k * GROUPS + g
            part = slice(g * rows, (g + 1) * rows)
            out_to(h, out[part])
            stats = jnp.where(lane == first + h, peak[part], stats)
            stats = jnp.where(lane == first + QH + h, total[part], stats)
    return stats


def exchange(
    n,
    cap,
    live,
    target,
    used,
    label_ref,
    q_ref,
    tk_ref,
    tv_ref,
    link_ref,
    pk_hbm,
    pv_hbm,
    attended,
    reads_ref,
    pk_ref,
    pv_ref,
    labels,
    label_now,
    got_out,
    got_stats,
    tree_out,
    tree_stats,
    q_all,
    q_now,
    out_send,
    stats_send,
    label_send_sem,
    label_recv_sem,
    q_send_sem,
    q_recv_sem,
    out_send_sem,
    out_recv_sem,
    stats_send_sem,
    stats_recv_sem,
    local_sem,
):
    reqs, tree, _ = q_ref.shape
    pages_here, page, _ = pk_ref.shape
    slots = target.shape[0] // reqs
    lanes = cap * 2 * QH
    fold = HD // lanes
    rows_held = tree // fold
    depth = n // 2
    me = lax.axis_index("pages")
    z, y = me // 2, me % 2
    other = 1 - y
    partner = z * 2 + other

    load_keys = pltpu.make_async_copy(pk_hbm, pk_ref, local_sem.at[2])
    load_values = pltpu.make_async_copy(pv_hbm, pv_ref, local_sem.at[3])
    load_keys.start()
    load_values.start()

    barrier = pltpu.get_barrier_semaphore()

    def greet(i, _):
        pl.semaphore_signal(
            barrier, inc=1, device_id={"pages": (me + i) % n}, device_id_type=MESH
        )
        return 0

    lax.fori_loop(1, n, greet, 0)
    pl.semaphore_wait(barrier, n - 1)

    def q_copy(src_ref, src, i, way, to):
        return pltpu.make_async_remote_copy(
            src_ref=src_ref,
            dst_ref=q_all.at[src, i],
            send_sem=q_send_sem.at[way, src // 2, i],
            recv_sem=q_recv_sem.at[src, i],
            device_id={"pages": to},
            device_id_type=MESH,
        )

    def out_copy(d):
        return pltpu.make_async_remote_copy(
            src_ref=out_send.at[d],
            dst_ref=got_out.at[pl.ds(me * cap, cap)],
            send_sem=out_send_sem.at[d],
            recv_sem=out_recv_sem.at[me],
            device_id={"pages": d},
            device_id_type=MESH,
        )

    def stats_copy(d):
        return pltpu.make_async_remote_copy(
            src_ref=stats_send.at[d],
            dst_ref=got_stats.at[me],
            send_sem=stats_send_sem.at[d],
            recv_sem=stats_recv_sem.at[me],
            device_id={"pages": d},
            device_id_type=MESH,
        )

    def q_arrive(src, i):
        pltpu.make_async_remote_copy(
            src_ref=q_all.at[src, i],
            dst_ref=q_all.at[src, i],
            send_sem=q_send_sem.at[0, src // 2, i],
            recv_sem=q_recv_sem.at[src, i],
            device_id={"pages": partner},
            device_id_type=MESH,
        ).wait_recv()

    def label_copy(d):
        return pltpu.make_async_remote_copy(
            src_ref=label_ref.at[d],
            dst_ref=labels.at[me],
            send_sem=label_send_sem.at[d],
            recv_sem=label_recv_sem.at[me],
            device_id={"pages": d},
            device_id_type=MESH,
        )

    def tell(i, _):
        label_copy((me + i) % n).start()
        return 0

    lax.fori_loop(1, n, tell, 0)

    for i in range(reqs):
        q_copy(q_ref.at[i], me, i, 2, partner).start()

        @pl.when(z + 1 < depth)
        def _():
            q_copy(q_ref.at[i], me, i, 0, me + 2).start()

        @pl.when(z > 0)
        def _():
            q_copy(q_ref.at[i], me, i, 1, me - 2).start()

    lane = lax.broadcasted_iota(jnp.int32, (tree, HD), 1)
    key_lane = lax.broadcasted_iota(jnp.int32, (GROUPS * tree, page), 1)

    def serve(d):
        stats = jnp.zeros((tree, HD), jnp.float32)
        for c in range(cap):
            which, count, req = (label_now[d, 0, c * 4 + f] for f in range(3))

            def out_to(h, value):
                out_send[d, c, :, head(h)] = value.astype(jnp.bfloat16)

            stats = attend(
                lambda h: q_now[req, :, head(h)],
                lambda k: pk_ref[which, :, head(k)],
                lambda k: pv_ref[which, :, head(k)],
                key_lane < count,
                out_to,
                stats,
                lane,
                c * 2 * QH,
            )
        stats_send[d] = jnp.concatenate(
            [stats[i * rows_held : (i + 1) * rows_held, :lanes] for i in range(fold)], axis=1
        )

    def one_tree(r, _):
        reach = link_ref[r]
        for level in range((tree - 1).bit_length()):
            reach = jnp.where(
                jnp.dot(reach, reach, preferred_element_type=jnp.float32) > 0, 1.0, 0.0
            ).astype(jnp.bfloat16)
        seen = lax.broadcasted_iota(jnp.int32, (tree, tree), 1) < live[r]
        open_ = jnp.where(seen, reach.astype(jnp.float32), 0.0)
        allowed = jnp.concatenate([open_] * GROUPS, axis=0) > 0

        def out_to(h, value):
            tree_out[r, :, head(h)] = value

        tree_stats[r] = attend(
            lambda h: q_ref[r, :, head(h)],
            lambda k: tk_ref[r, :, head(k)],
            lambda k: tv_ref[r, :, head(k)],
            allowed,
            out_to,
            jnp.zeros((tree, HD), jnp.float32),
            lane,
            0,
        )
        return 0

    lax.fori_loop(0, reqs, one_tree, 0)

    labels[me] = label_ref[me]

    def hear(i, _):
        d = (me + i) % n
        pltpu.make_async_remote_copy(
            src_ref=label_ref.at[d],
            dst_ref=labels.at[d],
            send_sem=label_send_sem.at[d],
            recv_sem=label_recv_sem.at[d],
            device_id={"pages": d},
            device_id_type=MESH,
        ).wait()
        return 0

    lax.fori_loop(1, n, hear, 0)
    into_scalars = pltpu.make_async_copy(labels, label_now, local_sem.at[0])
    into_scalars.start()
    into_scalars.wait()
    load_keys.wait()
    load_values.wait()

    q_now[...] = q_ref[...]
    serve(me)
    for c in range(cap):
        got_out[me * cap + c] = out_send[me, c]
    got_stats[me] = stats_send[me]

    page_row = lax.broadcasted_iota(jnp.int32, (pages_here, HD), 0)

    def count_reads(d, reads):
        for c in range(cap):
            which, count, _, lives = (label_now[d, 0, c * 4 + f] for f in range(4))
            lives = jnp.where(count > 0, lives, 0)
            reads = reads + jnp.where(page_row == which, lives, 0)
        return reads

    reads_ref[...] = lax.fori_loop(
        0, n, count_reads, jnp.zeros((pages_here, HD), jnp.int32)
    )

    def step(s, _):
        for i in range(reqs):

            @pl.when(z - s >= 0)
            def _():
                src = me - 2 * s
                q_arrive(src, i)
                q_copy(q_all.at[src, i], src, i, 2, partner).start()

                @pl.when(z + 1 < depth)
                def _():
                    q_copy(q_all.at[src, i], src, i, 0, me + 2).start()

            @pl.when(z + s < depth)
            def _():
                src = me + 2 * s
                q_arrive(src, i)
                q_copy(q_all.at[src, i], src, i, 2, partner).start()

                @pl.when(z > 0)
                def _():
                    q_copy(q_all.at[src, i], src, i, 1, me - 2).start()

        def case(k, _):
            crossed = k // 2
            far = s - crossed
            row = z + far * (2 * (k % 2) - 1)
            column = y + crossed * (other - y)
            d = row * 2 + column
            valid = (row >= 0) & (row < depth) & ((far > 0) | (k == 2))

            @pl.when(valid)
            def _():
                @pl.when(crossed == 1)
                def _():
                    for i in range(reqs):
                        q_arrive(d, i)

                q_now[...] = q_all[d]
                serve(d)
                out_copy(d).start()
                stats_copy(d).start()

            return 0

        lax.fori_loop(0, 4, case, 0)
        return 0

    lax.fori_loop(1, depth + 1, step, 0)

    def finish(i, _):
        d = (me + i) % n
        out_copy(d).wait_send()
        stats_copy(d).wait_send()
        pltpu.make_async_remote_copy(
            src_ref=out_send.at[d],
            dst_ref=got_out.at[pl.ds(d * cap, cap)],
            send_sem=out_send_sem.at[d],
            recv_sem=out_recv_sem.at[d],
            device_id={"pages": d},
            device_id_type=MESH,
        ).wait_recv()
        pltpu.make_async_remote_copy(
            src_ref=stats_send.at[d],
            dst_ref=got_stats.at[d],
            send_sem=stats_send_sem.at[d],
            recv_sem=stats_recv_sem.at[d],
            device_id={"pages": d},
            device_id_type=MESH,
        ).wait_recv()
        return 0

    lax.fori_loop(1, n, finish, 0)

    def drain(row, _):
        src = row * 2 + y
        for i in range(reqs):
            q_copy(q_all.at[src, i], src, i, 2, partner).wait_send()

            @pl.when((row <= z) & (z + 1 < depth))
            def _():
                q_copy(q_all.at[src, i], src, i, 0, me + 2).wait_send()

            @pl.when((row >= z) & (z > 0))
            def _():
                q_copy(q_all.at[src, i], src, i, 1, me - 2).wait_send()

        return 0

    lax.fori_loop(0, depth, drain, 0)

    def merge(r, _):
        tree_peak, tree_total = tree_stats[r, :, :QH], tree_stats[r, :, QH : 2 * QH]
        top = tree_peak
        peaks, totals = [], []
        for j in range(slots):
            where_ = target[r * slots + j]
            live_slot = used[r * slots + j] > 0
            packed = got_stats[where_ // cap]
            held = jnp.concatenate(
                [packed[:, i * lanes : (i + 1) * lanes] for i in range(fold)], axis=0
            )
            mine = held[:, : 2 * QH]
            for c in range(1, cap):
                mine = jnp.where(
                    where_ % cap == c, held[:, c * 2 * QH : (c + 1) * 2 * QH], mine
                )
            peaks.append(jnp.where(live_slot, mine[:, :QH], NEG_BIG))
            totals.append(mine[:, QH:])
            top = jnp.maximum(top, peaks[j])
        tree_scale = jnp.exp(tree_peak - top)
        scales = [
            jnp.where(used[r * slots + j] > 0, jnp.exp(peaks[j] - top), 0.0)
            for j in range(slots)
        ]
        total = tree_total * tree_scale
        for j in range(slots):
            total = total + scales[j] * totals[j]
        tree_scale = tree_scale / total
        scales = [scale / total for scale in scales]
        for h in range(QH):
            mixed = tree_out[r, :, head(h)] * tree_scale[:, h : h + 1]
            for j in range(slots):
                part = got_out[target[r * slots + j], :, head(h)].astype(jnp.float32)
                mixed = mixed + part * scales[j][:, h : h + 1]
            attended[r, :, head(h)] = mixed.astype(jnp.bfloat16)
        return 0

    lax.fori_loop(0, reqs, merge, 0)


def shards(
    queries,
    tree_keys,
    tree_values,
    page_keys,
    page_values,
    page_table,
    prefix_lengths,
    tree_parents,
    live_lengths,
):
    n = lax.axis_size("pages")
    me = lax.axis_index("pages")
    reqs, tree, width = queries.shape
    pages_here, page_size, _ = page_keys.shape
    slots = page_table.shape[1]
    pairs = reqs * slots
    cap = max(1, pairs // n)

    pair = jnp.arange(pairs, dtype=jnp.int32)
    my_pages = page_table.reshape(-1)
    my_counts = jnp.clip(
        jnp.repeat(prefix_lengths, slots) - pair % slots * page_size, 0, page_size
    )
    my_used = my_counts > 0
    owners = my_pages // pages_here
    before = pair[None, :] < pair[:, None]
    rank = jnp.sum(
        ((owners[:, None] == owners[None, :]) & my_used[None, :] & before).astype(jnp.int32),
        axis=1,
    )
    target = jnp.where(my_used, owners * cap + rank, me * cap)
    used = my_used.astype(jnp.int32)
    facts = jnp.stack(
        [my_pages % pages_here, my_counts, pair // slots, jnp.repeat(live_lengths, slots)]
    )
    place = jnp.arange(n * cap, dtype=jnp.int32)
    take = my_used[None, :] & (target[None, :] == place[:, None])
    labels = jnp.sum(jnp.where(take[:, None, :], facts[None], 0), axis=2)
    labels = jnp.pad(labels.reshape(n, 1, cap * 4), ((0, 0), (0, 7), (0, HD - cap * 4)))

    index = jnp.arange(tree, dtype=jnp.int32)
    links = (
        (index[None, None, :] == tree_parents[:, :, None])
        | (index[None, :, None] == index[None, None, :])
    ).astype(jnp.bfloat16)

    smem = pl.BlockSpec(memory_space=pltpu.SMEM)
    vmem = pl.BlockSpec(memory_space=pltpu.VMEM)
    hbm = pl.BlockSpec(memory_space=pl.ANY)
    depth = n // 2
    held_stats = (n, tree * cap * 2 * QH // HD, HD)
    attended, reads = pl.pallas_call(
        functools.partial(exchange, n, cap),
        out_shape=(
            jax.ShapeDtypeStruct((reqs, tree, width), jnp.bfloat16),
            jax.ShapeDtypeStruct((pages_here, HD), jnp.int32),
        ),
        in_specs=[smem] * 3 + [vmem] * 5 + [hbm] * 2,
        out_specs=(vmem, vmem),
        scratch_shapes=[
            pltpu.VMEM(page_keys.shape, jnp.bfloat16),
            pltpu.VMEM(page_values.shape, jnp.bfloat16),
            pltpu.VMEM((n, 8, HD), jnp.int32),
            pltpu.SMEM((n, 8, HD), jnp.int32),
            pltpu.VMEM((n * cap, tree, width), jnp.bfloat16),
            pltpu.VMEM(held_stats, jnp.float32),
            pltpu.VMEM((reqs, tree, width), jnp.float32),
            pltpu.VMEM((reqs, tree, HD), jnp.float32),
            pltpu.VMEM((n, reqs, tree, width), jnp.bfloat16),
            pltpu.VMEM((reqs, tree, width), jnp.bfloat16),
            pltpu.VMEM((n, cap, tree, width), jnp.bfloat16),
            pltpu.VMEM(held_stats, jnp.float32),
            pltpu.SemaphoreType.DMA((n,)),
            pltpu.SemaphoreType.DMA((n,)),
            pltpu.SemaphoreType.DMA((3, depth, reqs)),
            pltpu.SemaphoreType.DMA((n, reqs)),
            pltpu.SemaphoreType.DMA((n,)),
            pltpu.SemaphoreType.DMA((n,)),
            pltpu.SemaphoreType.DMA((n,)),
            pltpu.SemaphoreType.DMA((n,)),
            pltpu.SemaphoreType.DMA((4,)),
        ],
        compiler_params=pltpu.CompilerParams(
            collective_id=0, has_side_effects=True, vmem_limit_bytes=63 * 1024 * 1024
        ),
        name="exchange",
    )(
        live_lengths,
        target,
        used,
        labels,
        queries,
        tree_keys,
        tree_values,
        links,
        page_keys,
        page_values,
    )
    return (attended, reads[:, 0])


def solution(mesh):
    rows = P(("grp", "pages"), None, None)
    return jax.shard_map(
        shards,
        mesh=mesh,
        in_specs=(
            rows,
            rows,
            rows,
            rows,
            rows,
            P(("grp", "pages"), None),
            P(("grp", "pages")),
            P(("grp", "pages"), None),
            P(("grp", "pages")),
        ),
        out_specs=(rows, P(("grp", "pages"))),
        check_vma=False,
    )
```

```python
import functools

import jax
import jax.numpy as jnp
from jax import lax
from jax.experimental import pallas as pl
from jax.experimental.pallas import tpu as pltpu
from jax.sharding import PartitionSpec as P

QH = 16
KVH = 4
HD = 128
GROUPS = QH // KVH
NEG_BIG = -1e30
SCALE = HD ** (-0.5)
NT = (((1,), (1,)), ((), ()))
MESH = pl.DeviceIdType.MESH


def head(h):
    return slice(h * HD, (h + 1) * HD)


def attend(query_of, keys_of, values_of, allowed, out_to, stats, lane, first):
    for k in range(KVH):
        query = jnp.concatenate([query_of(k * GROUPS + g) for g in range(GROUPS)], axis=0)
        scores = (
            lax.dot_general(query, keys_of(k), NT, preferred_element_type=jnp.float32) * SCALE
        )
        scores = jnp.where(allowed, scores, NEG_BIG)
        peak = jnp.max(scores, axis=-1, keepdims=True)
        expo = jnp.exp(scores - peak)
        total = jnp.sum(expo, axis=-1, keepdims=True)
        out = jnp.dot(
            expo.astype(jnp.bfloat16), values_of(k), preferred_element_type=jnp.float32
        )
        rows = out.shape[0] // GROUPS
        for g in range(GROUPS):
            h = k * GROUPS + g
            part = slice(g * rows, (g + 1) * rows)
            out_to(h, out[part])
            stats = jnp.where(lane == first + h, peak[part], stats)
            stats = jnp.where(lane == first + QH + h, total[part], stats)
    return stats


def exchange(
    n,
    cap,
    table,
    prefix,
    live,
    parents_ref,
    q_ref,
    tk_ref,
    tv_ref,
    pk_hbm,
    pv_hbm,
    attended,
    reads_ref,
    pk_ref,
    pv_ref,
    target,
    used,
    label_ref,
    labels,
    label_now,
    got_out,
    got_stats,
    tree_out,
    tree_stats,
    q_all,
    q_now,
    out_send,
    stats_send,
    label_send_sem,
    label_recv_sem,
    q_send_sem,
    q_recv_sem,
    out_send_sem,
    out_recv_sem,
    stats_send_sem,
    stats_recv_sem,
    local_sem,
):
    reqs, tree, _ = q_ref.shape
    pages_here, page, _ = pk_ref.shape
    slots = table.shape[1]
    lanes = cap * 2 * QH
    fold = HD // lanes
    rows_held = tree // fold
    depth = n // 2
    me = lax.axis_index("pages")
    z, y = me // 2, me % 2
    other = 1 - y
    partner = z * 2 + other

    load_keys = pltpu.make_async_copy(pk_hbm, pk_ref, local_sem.at[2])
    load_values = pltpu.make_async_copy(pv_hbm, pv_ref, local_sem.at[3])
    load_keys.start()
    load_values.start()

    barrier = pltpu.get_barrier_semaphore()

    def greet(i, _):
        pl.semaphore_signal(
            barrier, inc=1, device_id={"pages": (me + i) % n}, device_id_type=MESH
        )
        return 0

    lax.fori_loop(1, n, greet, 0)
    pl.semaphore_wait(barrier, n - 1)

    def q_copy(src_ref, src, i, way, to):
        return pltpu.make_async_remote_copy(
            src_ref=src_ref,
            dst_ref=q_all.at[src, i],
            send_sem=q_send_sem.at[way, src // 2, i],
            recv_sem=q_recv_sem.at[src, i],
            device_id={"pages": to},
            device_id_type=MESH,
        )

    def out_copy(d):
        return pltpu.make_async_remote_copy(
            src_ref=out_send.at[d],
            dst_ref=got_out.at[pl.ds(me * cap, cap)],
            send_sem=out_send_sem.at[d],
            recv_sem=out_recv_sem.at[me],
            device_id={"pages": d},
            device_id_type=MESH,
        )

    def stats_copy(d):
        return pltpu.make_async_remote_copy(
            src_ref=stats_send.at[d],
            dst_ref=got_stats.at[me],
            send_sem=stats_send_sem.at[d],
            recv_sem=stats_recv_sem.at[me],
            device_id={"pages": d},
            device_id_type=MESH,
        )

    def q_arrive(src, i):
        pltpu.make_async_remote_copy(
            src_ref=q_all.at[src, i],
            dst_ref=q_all.at[src, i],
            send_sem=q_send_sem.at[0, src // 2, i],
            recv_sem=q_recv_sem.at[src, i],
            device_id={"pages": partner},
            device_id_type=MESH,
        ).wait_recv()

    for i in range(reqs):
        q_copy(q_ref.at[i], me, i, 2, partner).start()

        @pl.when(z + 1 < depth)
        def _():
            q_copy(q_ref.at[i], me, i, 0, me + 2).start()

        @pl.when(z > 0)
        def _():
            q_copy(q_ref.at[i], me, i, 1, me - 2).start()

    label_row = lax.broadcasted_iota(jnp.int32, (n, HD), 0)
    label_lane = lax.broadcasted_iota(jnp.int32, (n, HD), 1)
    told = jnp.zeros((n, HD), jnp.int32)
    owners, taken = [], []
    for p in range(reqs * slots):
        r, j = p // slots, p % slots
        count = jnp.clip(prefix[r] - j * page, 0, page)
        owner = lax.div(table[r, j], jnp.int32(pages_here))
        rank = jnp.int32(0)
        for earlier in range(p):
            same = (owners[earlier] == owner) & (taken[earlier] > 0)
            rank = rank + jnp.where(same, 1, 0)
        takes = jnp.where(count > 0, 1, 0)
        owners.append(owner)
        taken.append(takes)
        used[p] = takes
        target[p] = jnp.where(count > 0, owner * cap + rank, me * cap)
        row = label_row == jnp.where(count > 0, owner, -1)
        facts = (table[r, j] - owner * pages_here, count, r, live[r])
        for f, fact in enumerate(facts):
            told = jnp.where(row & (label_lane == rank * 4 + f), fact, told)
    for d in range(n):
        label_ref[d, 0:1, :] = told[d : d + 1]

    def label_copy(d):
        return pltpu.make_async_remote_copy(
            src_ref=label_ref.at[d],
            dst_ref=labels.at[me],
            send_sem=label_send_sem.at[d],
            recv_sem=label_recv_sem.at[me],
            device_id={"pages": d},
            device_id_type=MESH,
        )

    def tell(i, _):
        label_copy((me + i) % n).start()
        return 0

    lax.fori_loop(1, n, tell, 0)

    lane = lax.broadcasted_iota(jnp.int32, (tree, HD), 1)
    key_lane = lax.broadcasted_iota(jnp.int32, (GROUPS * tree, page), 1)

    def serve(d):
        stats = jnp.zeros((tree, HD), jnp.float32)
        for c in range(cap):
            which, count, req = (label_now[d, 0, c * 4 + f] for f in range(3))

            def out_to(h, value):
                out_send[d, c, :, head(h)] = value.astype(jnp.bfloat16)

            stats = attend(
                lambda h: q_now[req, :, head(h)],
                lambda k: pk_ref[which, :, head(k)],
                lambda k: pv_ref[which, :, head(k)],
                key_lane < count,
                out_to,
                stats,
                lane,
                c * 2 * QH,
            )
        stats_send[d] = jnp.concatenate(
            [stats[i * rows_held : (i + 1) * rows_held, :lanes] for i in range(fold)], axis=1
        )

    def one_tree(r, _):
        source = lax.broadcasted_iota(jnp.int32, (tree, tree), 0)
        child = lax.broadcasted_iota(jnp.int32, (tree, tree), 1)
        linked = (source == parents_ref[pl.ds(r, 1), :]) | (source == child)
        same = jnp.where(source == child, 1.0, 0.0).astype(jnp.bfloat16)
        reach = jnp.where(linked, 1.0, 0.0).astype(jnp.bfloat16)
        for level in range((tree - 1).bit_length()):
            reach = jnp.where(
                jnp.dot(reach, reach, preferred_element_type=jnp.float32) > 0, 1.0, 0.0
            ).astype(jnp.bfloat16)
        upright = lax.dot_general(
            reach, same, (((0,), (0,)), ((), ())), preferred_element_type=jnp.float32
        )
        open_ = jnp.where(child < live[r], upright, 0.0)
        allowed = jnp.concatenate([open_] * GROUPS, axis=0) > 0

        def out_to(h, value):
            tree_out[r, :, head(h)] = value

        tree_stats[r] = attend(
            lambda h: q_ref[r, :, head(h)],
            lambda k: tk_ref[r, :, head(k)],
            lambda k: tv_ref[r, :, head(k)],
            allowed,
            out_to,
            jnp.zeros((tree, HD), jnp.float32),
            lane,
            0,
        )
        return 0

    lax.fori_loop(0, reqs, one_tree, 0)

    labels[me] = label_ref[me]

    def hear(i, _):
        d = (me + i) % n
        pltpu.make_async_remote_copy(
            src_ref=label_ref.at[d],
            dst_ref=labels.at[d],
            send_sem=label_send_sem.at[d],
            recv_sem=label_recv_sem.at[d],
            device_id={"pages": d},
            device_id_type=MESH,
        ).wait()
        return 0

    lax.fori_loop(1, n, hear, 0)
    into_scalars = pltpu.make_async_copy(labels, label_now, local_sem.at[0])
    into_scalars.start()
    into_scalars.wait()
    load_keys.wait()
    load_values.wait()

    q_now[...] = q_ref[...]
    serve(me)
    for c in range(cap):
        got_out[me * cap + c] = out_send[me, c]
    got_stats[me] = stats_send[me]

    page_row = lax.broadcasted_iota(jnp.int32, (pages_here, HD), 0)

    def count_reads(d, reads):
        for c in range(cap):
            which, count, _, lives = (label_now[d, 0, c * 4 + f] for f in range(4))
            lives = jnp.where(count > 0, lives, 0)
            reads = reads + jnp.where(page_row == which, lives, 0)
        return reads

    reads_ref[...] = lax.fori_loop(
        0, n, count_reads, jnp.zeros((pages_here, HD), jnp.int32)
    )

    def step(s, _):
        for i in range(reqs):

            @pl.when(z - s >= 0)
            def _():
                src = me - 2 * s
                q_arrive(src, i)
                q_copy(q_all.at[src, i], src, i, 2, partner).start()

                @pl.when(z + 1 < depth)
                def _():
                    q_copy(q_all.at[src, i], src, i, 0, me + 2).start()

            @pl.when(z + s < depth)
            def _():
                src = me + 2 * s
                q_arrive(src, i)
                q_copy(q_all.at[src, i], src, i, 2, partner).start()

                @pl.when(z > 0)
                def _():
                    q_copy(q_all.at[src, i], src, i, 1, me - 2).start()

        def case(k, _):
            crossed = k // 2
            far = s - crossed
            row = z + far * (2 * (k % 2) - 1)
            column = y + crossed * (other - y)
            d = row * 2 + column
            valid = (row >= 0) & (row < depth) & ((far > 0) | (k == 2))

            @pl.when(valid)
            def _():
                @pl.when(crossed == 1)
                def _():
                    for i in range(reqs):
                        q_arrive(d, i)

                q_now[...] = q_all[d]
                serve(d)
                out_copy(d).start()
                stats_copy(d).start()

            return 0

        lax.fori_loop(0, 4, case, 0)
        return 0

    lax.fori_loop(1, depth + 1, step, 0)

    def finish(i, _):
        d = (me + i) % n
        out_copy(d).wait_send()
        stats_copy(d).wait_send()
        pltpu.make_async_remote_copy(
            src_ref=out_send.at[d],
            dst_ref=got_out.at[pl.ds(d * cap, cap)],
            send_sem=out_send_sem.at[d],
            recv_sem=out_recv_sem.at[d],
            device_id={"pages": d},
            device_id_type=MESH,
        ).wait_recv()
        pltpu.make_async_remote_copy(
            src_ref=stats_send.at[d],
            dst_ref=got_stats.at[d],
            send_sem=stats_send_sem.at[d],
            recv_sem=stats_recv_sem.at[d],
            device_id={"pages": d},
            device_id_type=MESH,
        ).wait_recv()
        return 0

    lax.fori_loop(1, n, finish, 0)

    def drain(row, _):
        src = row * 2 + y
        for i in range(reqs):
            q_copy(q_all.at[src, i], src, i, 2, partner).wait_send()

            @pl.when((row <= z) & (z + 1 < depth))
            def _():
                q_copy(q_all.at[src, i], src, i, 0, me + 2).wait_send()

            @pl.when((row >= z) & (z > 0))
            def _():
                q_copy(q_all.at[src, i], src, i, 1, me - 2).wait_send()

        return 0

    lax.fori_loop(0, depth, drain, 0)

    def merge(r, _):
        tree_peak, tree_total = tree_stats[r, :, :QH], tree_stats[r, :, QH : 2 * QH]
        top = tree_peak
        peaks, totals = [], []
        for j in range(slots):
            where_ = target[r * slots + j]
            live_slot = used[r * slots + j] > 0
            packed = got_stats[where_ // cap]
            held = jnp.concatenate(
                [packed[:, i * lanes : (i + 1) * lanes] for i in range(fold)], axis=0
            )
            mine = held[:, : 2 * QH]
            for c in range(1, cap):
                mine = jnp.where(
                    where_ % cap == c, held[:, c * 2 * QH : (c + 1) * 2 * QH], mine
                )
            peaks.append(jnp.where(live_slot, mine[:, :QH], NEG_BIG))
            totals.append(mine[:, QH:])
            top = jnp.maximum(top, peaks[j])
        tree_scale = jnp.exp(tree_peak - top)
        scales = [
            jnp.where(used[r * slots + j] > 0, jnp.exp(peaks[j] - top), 0.0)
            for j in range(slots)
        ]
        total = tree_total * tree_scale
        for j in range(slots):
            total = total + scales[j] * totals[j]
        tree_scale = tree_scale / total
        scales = [scale / total for scale in scales]
        for h in range(QH):
            mixed = tree_out[r, :, head(h)] * tree_scale[:, h : h + 1]
            for j in range(slots):
                part = got_out[target[r * slots + j], :, head(h)].astype(jnp.float32)
                mixed = mixed + part * scales[j][:, h : h + 1]
            attended[r, :, head(h)] = mixed.astype(jnp.bfloat16)
        return 0

    lax.fori_loop(0, reqs, merge, 0)


def shards(
    queries,
    tree_keys,
    tree_values,
    page_keys,
    page_values,
    page_table,
    prefix_lengths,
    tree_parents,
    live_lengths,
):
    n = lax.axis_size("pages")
    reqs, tree, width = queries.shape
    pages_here = page_keys.shape[0]
    slots = page_table.shape[1]
    pairs = reqs * slots
    cap = max(1, pairs // n)

    smem = pl.BlockSpec(memory_space=pltpu.SMEM)
    vmem = pl.BlockSpec(memory_space=pltpu.VMEM)
    hbm = pl.BlockSpec(memory_space=pl.ANY)
    depth = n // 2
    held_stats = (n, tree * cap * 2 * QH // HD, HD)
    attended, reads = pl.pallas_call(
        functools.partial(exchange, n, cap),
        out_shape=(
            jax.ShapeDtypeStruct((reqs, tree, width), jnp.bfloat16),
            jax.ShapeDtypeStruct((pages_here, HD), jnp.int32),
        ),
        in_specs=[smem] * 3 + [vmem] * 4 + [hbm] * 2,
        out_specs=(vmem, vmem),
        scratch_shapes=[
            pltpu.VMEM(page_keys.shape, jnp.bfloat16),
            pltpu.VMEM(page_values.shape, jnp.bfloat16),
            pltpu.SMEM((pairs,), jnp.int32),
            pltpu.SMEM((pairs,), jnp.int32),
            pltpu.VMEM((n, 8, HD), jnp.int32),
            pltpu.VMEM((n, 8, HD), jnp.int32),
            pltpu.SMEM((n, 8, HD), jnp.int32),
            pltpu.VMEM((n * cap, tree, width), jnp.bfloat16),
            pltpu.VMEM(held_stats, jnp.float32),
            pltpu.VMEM((reqs, tree, width), jnp.float32),
            pltpu.VMEM((reqs, tree, HD), jnp.float32),
            pltpu.VMEM((n, reqs, tree, width), jnp.bfloat16),
            pltpu.VMEM((reqs, tree, width), jnp.bfloat16),
            pltpu.VMEM((n, cap, tree, width), jnp.bfloat16),
            pltpu.VMEM(held_stats, jnp.float32),
            pltpu.SemaphoreType.DMA((n,)),
            pltpu.SemaphoreType.DMA((n,)),
            pltpu.SemaphoreType.DMA((3, depth, reqs)),
            pltpu.SemaphoreType.DMA((n, reqs)),
            pltpu.SemaphoreType.DMA((n,)),
            pltpu.SemaphoreType.DMA((n,)),
            pltpu.SemaphoreType.DMA((n,)),
            pltpu.SemaphoreType.DMA((n,)),
            pltpu.SemaphoreType.DMA((4,)),
        ],
        compiler_params=pltpu.CompilerParams(
            collective_id=0, has_side_effects=True, vmem_limit_bytes=63 * 1024 * 1024
        ),
        name="exchange",
    )(
        page_table,
        prefix_lengths,
        live_lengths,
        tree_parents,
        queries,
        tree_keys,
        tree_values,
        page_keys,
        page_values,
    )
    return (attended, reads[:, 0])


def solution(mesh):
    rows = P(("grp", "pages"), None, None)
    return jax.shard_map(
        shards,
        mesh=mesh,
        in_specs=(
            rows,
            rows,
            rows,
            rows,
            rows,
            P(("grp", "pages"), None),
            P(("grp", "pages")),
            P(("grp", "pages"), None),
            P(("grp", "pages")),
        ),
        out_specs=(rows, P(("grp", "pages"))),
        check_vma=False,
    )
```
